32 devices in a mesh: dp: 4 (over x, core), expert: 4 (over z), etp: 2 (over y).
Axes of the slice: x: 2, y: 2, z: 4, core: 2. Of those that a mesh axis runs over, the one named last changes fastest.
Arguments:
- tokens: bfloat16 [4096, 3072], P(('dp', 'expert'), 'etp'), parts along dimension 0, may hold values from -6 to 6
- experts: int32 [4096, 2], P(('dp', 'expert')), parts along dimension 0, may hold values from 0 to 3, all different within a row; in each aligned block of 256 rows (0 to 255, 256 to 511, ...) at most 176 rows name the same one
- mixing: float32 [4096, 2], P(('dp', 'expert')), parts along dimension 0, may hold values from 0.2 to 1
- up_weight: bfloat16 [4, 3072, 8192], P('expert', None, 'etp'), may hold values from -0.109375 to 0.109375
- down_weight: bfloat16 [4, 8192, 3072], P('expert', 'etp'), may hold values from -0.0625 to 0.0625
Outputs:
- mixed: bfloat16 [4096, 3072], P(('dp', 'expert'), 'etp'), parts along dimension 0
The draws below stay inside these ranges and needn't reach their ends.
There are 4 independent parts, one for each index of `dp`. The reference program is written for one: setup_inputs(seed, part) draws one part's arguments, and reference() takes and returns one part's arrays. A program takes and returns all parts, laid end to end along the dimension named above; an argument that names none is the same for every part. Nothing has to cross between parts.
Inputs may be any that keep to these rules, and one draw needn't show every extreme that they name: Each row names two different experts. In the rows of one index of expert (aligned blocks of 256 rows) no expert is named more than 176 times, a bound that some block reaches.
All inputs are finite; a program needn't handle non-finite values.
Results may differ from the reference program's by a relative error of at most 0.0078.
Values may be sent and summed in bfloat16 or wider, within the bound.
No kernel may reach another device: no remote copies, remote signals or barrier semaphores. Data moves between devices by JAX's collectives and lax.ppermute only.
A program may use at most 128 MiB of HBM per device.

```python
import math
import jax
import jax.numpy as jnp
import numpy as np
from jax import lax

D = 3072
FF = 8192
TOK_DEV = 256
E = 4
CAP = 176
TOKENS = 1024


def shard_levels(own_key, shape, pieces, low, high):
    factor_of, own = 1.0, jax.random.fold_in(own_key, 6)
    for position, parts in pieces:
        draws = jnp.exp(jax.random.uniform(jax.random.fold_in(own, position), (parts,), jnp.float32, low / len(pieces), high / len(pieces)))
        factor_of = factor_of * jnp.repeat(draws, shape[position] // parts).reshape([-1 if axis == position else 1 for axis in range(len(shape))])
    return factor_of


def deal_out(stream_key, own, number, rows, amount, top, most, skew):
    ranking = jax.random.permutation(stream_key, amount)
    packed, usual = shares(amount, rows * top, most, skew, True), shares(amount, rows * top, most, skew, False)
    places = jnp.arange(amount)

    def named(lengths, offset_by):
        used = int((lengths > 0).sum())
        fixed = max(1, used // 4)
        moved = fixed + (places - fixed + offset_by * (used - fixed)) % max(1, amount - fixed)
        return jnp.zeros((amount,), jnp.int32).at[ranking[jnp.where(places < fixed, places, moved)]].set(jnp.asarray(lengths, jnp.int32))

    lengths = jnp.where(number % 4 == 0, named(packed, number // 4), named(usual, number - number // 4 - 1))
    mixed = jax.random.permutation(jax.random.fold_in(own, 3), amount)
    giver, sink = mixed[0:amount // 2 * 2:2], mixed[1:amount // 2 * 2:2]
    room = jnp.minimum(lengths[giver] - 1, most - lengths[sink]) // 2
    room = jnp.where((giver == ranking[0]) | (sink == ranking[0]) | (lengths[sink] == 0), 0, jnp.maximum(room, 0))
    moved = jax.random.randint(jax.random.fold_in(own, 4), (amount // 2,), 0, 1 << 20) % (room + 1)
    lengths = lengths.at[giver].add(-moved).at[sink].add(moved)
    members = jnp.searchsorted(jnp.cumsum(lengths), jnp.arange(rows * top), side="right").astype(jnp.int32)
    grid = members.reshape(top, rows).T
    grid = grid[jax.random.permutation(jax.random.fold_in(own, 1), rows)]
    offset_by = jax.random.randint(jax.random.fold_in(own, 2), (rows, 1), 0, top)
    return jnp.take_along_axis(grid, (jnp.arange(top)[None, :] + offset_by) % top, axis=1)


def shares(count, total, reach, skew, full):
    weights = [(1 << 20) // math.isqrt(grade ** skew) + 1 for grade in range(1, count + 1)]
    largest = reach if full else min(reach, max(-(-total // count), total * weights[0] // sum(weights)))
    least = 1 if total - largest >= count - 1 else 0
    holding, spare = [largest] + [least] * (count - 1), total - largest - least * (count - 1)
    while spare > 0:
        candidates = [i for i in range(1, count) if holding[i] < largest] or [i for i in range(1, count) if holding[i] < reach]
        whole, budget = sum([weights[i] for i in candidates]), spare
        for i in candidates:
            extra = min(reach - holding[i], max(1, budget * weights[i] // whole), spare)
            holding[i] = holding[i] + extra
            spare = spare - extra
    return np.array(holding)


def gaussian(key, extent, spread, reach, pieces=(), kind=jnp.bfloat16):
    entries = spread * jax.random.normal(key, extent, jnp.float32)
    if pieces:
        entries = entries * shard_levels(key, extent, pieces, -0.22, 0.18)
    return jnp.clip(entries, -reach, reach).astype(kind)


def setup_inputs(seed: int = 0, part: int = 0) -> dict:
    key_of = jax.random.split(jax.random.key(seed), 6)
    part_splits = jax.random.split(jax.random.fold_in(key_of[5], part), 6)
    tokens = gaussian(part_splits[0], (TOKENS, D), 1.0, 6.0, ((0, 4), (1, 2)))
    experts_keys = jax.random.split(jax.random.fold_in(part_splits[1], 1), TOKENS // TOK_DEV)
    experts_turns = jax.random.permutation(jax.random.fold_in(part_splits[1], 3), TOKENS // TOK_DEV)
    experts = jax.vmap(lambda own, number: deal_out(jax.random.fold_in(part_splits[1], 2), own, number, TOK_DEV, E, 2, CAP, 2))(experts_keys, experts_turns).reshape((TOKENS, 2))
    mixing = jnp.clip(0.2 + 0.8 * jax.random.uniform(part_splits[2], (TOKENS, 2), jnp.float32) ** shard_levels(part_splits[2], (TOKENS, 2), ((0, 4),), -0.2, 0.2), 0.2, 1.0)
    up_weight = gaussian(key_of[3], (E, D, FF), D ** -0.5, 0.109375, ((0, 4), (2, 2)))
    down_weight = gaussian(key_of[4], (E, FF, D), FF ** -0.5, 0.0625, ((0, 4), (1, 2)))
    return dict(tokens=tokens, experts=experts, mixing=mixing, up_weight=up_weight, down_weight=down_weight)


def reference(tokens, experts, mixing, up_weight, down_weight):
    flat_ids = experts.reshape(-1).astype(jnp.int32)
    assigned = flat_ids.shape[0]
    ordering = jnp.arange(assigned, dtype=jnp.int32)
    capacity = CAP * (TOKENS // TOK_DEV)
    flat_mix = mixing.reshape(-1)

    def one_expert(expert):
        sort_key = jnp.where(flat_ids == expert, 0, assigned).astype(jnp.int32) + ordering
        picked = jnp.argsort(sort_key)[:capacity].astype(jnp.int32)
        is_live = flat_ids[picked] == expert
        chosen_rows = tokens[picked // 2]
        up_proj = jnp.dot(chosen_rows, up_weight[expert], preferred_element_type=jnp.float32)
        hidden = jax.nn.silu(up_proj).astype(jnp.bfloat16)
        expert_out = jnp.dot(hidden, down_weight[expert], preferred_element_type=jnp.float32).astype(jnp.bfloat16)
        scaled = jnp.where(is_live, flat_mix[picked], jnp.zeros_like(flat_mix[picked]))
        return expert_out.astype(jnp.float32) * scaled[:, None], picked

    terms, picked = lax.map(one_expert, jnp.arange(E, dtype=jnp.int32))
    mixed = jnp.zeros((TOKENS, D), jnp.float32).at[(picked // 2).reshape(-1)].add(terms.reshape(-1, D))
    return mixed.astype(jnp.bfloat16)
```

```python
import jax
import jax.numpy as jnp
from jax import lax
from jax.sharding import PartitionSpec as P


def positions(chosen, expert_count):
    flat_ids = chosen.reshape(-1)
    one_hot = (flat_ids[:, None] == jnp.arange(expert_count, dtype=jnp.int32)[None, :]).astype(
        jnp.int32
    )
    before = jnp.cumsum(one_hot, axis=0) - one_hot
    return jnp.sum(before * one_hot, axis=1).reshape(chosen.shape)


def one_hot_rows(slot_ids, slot_total):
    return (
        slot_ids[:, :, None] == jnp.arange(slot_total, dtype=jnp.int32)[None, None, :]
    ).astype(jnp.bfloat16)


def local(tokens, experts, mixing, up_weight, down_weight):
    tok_rows = experts.shape[0]
    width = tokens.shape[1]
    groups = lax.axis_size("expert")
    halves = lax.axis_size("etp")
    capacity = 2 * tok_rows // groups * 11 // 8
    slot_total = groups * capacity
    up_slab = up_weight[0]
    down_slab = down_weight[0]
    me = lax.axis_index("expert")
    part = lax.axis_index("etp")

    def partner(offset):
        return [(i, i ^ offset) for i in range(groups)]

    def across(rows, offset):
        return rows if offset == 0 else lax.ppermute(rows, "expert", partner(offset))

    def join(rows):
        if halves != 2:
            return lax.all_gather(rows, "etp", axis=1, tiled=True)
        other = lax.ppermute(rows, "etp", [(0, 1), (1, 0)])
        first = jnp.where(part == 0, rows, other)
        second = jnp.where(part == 0, other, rows)
        return jnp.concatenate([first, second], axis=1)

    def reduce(sums):
        if halves != 2:
            return lax.psum_scatter(sums, "etp", scatter_dimension=1, tiled=True).astype(
                jnp.bfloat16
            )
        first, second = sums[:, :width], sums[:, width:]
        keep = jnp.where(part == 0, first, second)
        send = jnp.where(part == 0, second, first).astype(jnp.bfloat16)
        other = lax.ppermute(send, "etp", [(0, 1), (1, 0)])
        return (keep + other.astype(jnp.float32)).astype(jnp.bfloat16)

    slot_ids = (experts ^ me) * capacity + positions(experts, groups)
    placing = one_hot_rows(slot_ids, slot_total)
    outgoing = jnp.einsum(
        "rs,rd->sd", jnp.sum(placing, axis=1), tokens, preferred_element_type=jnp.float32
    ).astype(jnp.bfloat16)
    order = sorted(range(groups), key=lambda k: (k != 0, -(k & -k), k))
    returned = {}
    for offset in order:
        rows = across(outgoing[offset * capacity : (offset + 1) * capacity], offset)
        gathered = join(rows)
        up_proj = jnp.dot(gathered, up_slab, preferred_element_type=jnp.float32)
        hidden = jax.nn.silu(up_proj).astype(jnp.bfloat16)
        sums = jnp.dot(hidden, down_slab, preferred_element_type=jnp.float32)
        returned[offset] = across(reduce(sums), offset)
    mixed = jnp.zeros((tok_rows, width), jnp.float32)
    for offset in order:
        cols = placing[:, :, offset * capacity : (offset + 1) * capacity]
        for k in range(2):
            mixed = mixed + mixing[:, k : k + 1] * jnp.dot(
                cols[:, k], returned[offset], preferred_element_type=jnp.float32
            )
    return mixed.astype(jnp.bfloat16)


def solution(mesh):
    placed = (
        P(("dp", "expert"), "etp"),
        P(("dp", "expert"), None),
        P(("dp", "expert"), None),
        P("expert", None, "etp"),
        P("expert", "etp", None),
    )
    return jax.shard_map(
        local, mesh=mesh, in_specs=placed, out_specs=P(("dp", "expert"), "etp"), check_vma=False
    )
```

```python
import functools
import math

import jax
import jax.numpy as jnp
from jax import lax
from jax.experimental import pallas as pl
from jax.experimental.pallas import tpu as pltpu
from jax.sharding import PartitionSpec as P


VMEM = pl.BlockSpec(memory_space=pltpu.VMEM)
ANY = pl.BlockSpec(memory_space=pl.ANY)
HBM = pl.BlockSpec(memory_space=pltpu.HBM)
GRANT = 12 * 1024 * 1024
BATCHES = (((0, 0), (2, 0)), ((2, 1), (1, 0)), ((3, 0), (3, 1)))
MIX = (2, 1, 0, 3)
SPLIT = {2: 2, 3: 2}
HOLD = ((2, 0),)


def hold(arrays):
    return [pltpu.with_memory_space_constraint(array, pltpu.VMEM) for array in arrays]


def call(body, outs, scratch=(), flops=0, moved=0, grant=GRANT, **specs):
    return pl.pallas_call(
        body,
        out_specs=[VMEM] * len(outs),
        out_shape=outs,
        scratch_shapes=scratch,
        compiler_params=pltpu.CompilerParams(vmem_limit_bytes=grant),
        cost_estimate=pl.CostEstimate(flops=flops, bytes_accessed=moved, transcendentals=0),
        **specs,
    )


def tile_of(size):
    for tile in (512, 384, 256, 128):
        if size % tile == 0:
            return tile
    return size


def send_kernel(layout, experts_ref, mixing_ref, tokens_ref, table_ref, *out_refs):
    capacity, pieces = layout
    rows = tokens_ref.shape[0]
    me = lax.axis_index("expert")
    first = experts_ref[0:1, :]
    second = experts_ref[1:2, :]
    earlier = lax.broadcasted_iota(jnp.int32, (rows, rows), 0) < lax.broadcasted_iota(
        jnp.int32, (rows, rows), 1
    )
    earlier = earlier.astype(jnp.float32).astype(jnp.bfloat16)
    offsets = sorted({start // capacity for start, _ in pieces})
    first_slot = jnp.zeros((1, rows), jnp.int32)
    second_slot = jnp.zeros((1, rows), jnp.int32)
    for offset in offsets:
        expert = me ^ offset
        named = (first == expert) | (second == expert)
        marks = jnp.broadcast_to(named.astype(jnp.float32), (16, rows)).astype(jnp.bfloat16)
        rank = jnp.dot(marks, earlier, preferred_element_type=jnp.float32)[0:1, :]
        slot = rank.astype(jnp.int32) + offset * capacity
        first_slot = jnp.where(first == expert, slot, first_slot)
        second_slot = jnp.where(second == expert, slot, second_slot)
        slot = jnp.where(named, slot, -1)
        for (start, size), out_ref in zip(pieces, out_refs):
            if start // capacity == offset:
                places = lax.broadcasted_iota(jnp.int32, (size, rows), 0) + start
                placing = (slot == places).astype(jnp.float32).astype(jnp.bfloat16)
                out_ref[...] = jnp.dot(
                    placing, tokens_ref[...], preferred_element_type=jnp.float32
                ).astype(out_ref.dtype)
    lines = [
        first_slot.astype(jnp.float32),
        second_slot.astype(jnp.float32),
        mixing_ref[0:1, :],
        mixing_ref[1:2, :],
        jnp.zeros((124, rows), jnp.float32),
    ]
    table_ref[...] = jnp.concatenate(lines, axis=0).T


def send_rows(experts, mixing, tokens, capacity, pieces):
    rows, width = tokens.shape
    outs = [jax.ShapeDtypeStruct((rows, 128), jnp.float32)]
    outs += [jax.ShapeDtypeStruct((size, width), tokens.dtype) for _, size in pieces]
    return call(
        functools.partial(send_kernel, (capacity, pieces)),
        outs,
        flops=2 * rows * width * sum(size for _, size in pieces),
        moved=4 * rows * width,
        grant=12 * 1024 * 1024,
    )(experts.T, mixing.T, tokens)


def column_copies(source_ref, held_ref, base, sems):
    size, tile = source_ref.shape[0], held_ref.shape[1]

    def copy(index):
        cols = pl.ds(pl.multiple_of(index * tile, tile), tile)
        rows = pl.ds(pl.multiple_of(base + index * size, math.gcd(base, size)), size)
        return pltpu.make_async_copy(source_ref.at[:, cols], held_ref.at[rows], sems.at[index])

    return copy, source_ref.shape[1] // tile


def load_kernel(up_ref, *refs):
    held_ref, sems = refs[-2:]
    copy, count = column_copies(up_ref, held_ref, 0, sems)
    for index in range(count):
        copy(index).start()
    for index in range(count):
        copy(index).wait()


def load(up_weight, down_weight, after):
    tile = tile_of(math.gcd(up_weight.shape[1], down_weight.shape[1] // 2))
    size = up_weight.size + down_weight.size
    source = pltpu.with_memory_space_constraint(up_weight, pltpu.HBM)
    return call(
        load_kernel,
        [pltpu.VMEM((size // tile, tile), up_weight.dtype)],
        [pltpu.SemaphoreType.DMA((up_weight.shape[1] // tile,))],
        moved=2 * up_weight.size,
        flops=8 * 10**9,
        in_specs=[HBM] + [ANY] * len(after),
    )(source, *after)[0]


def expert_kernel(sizes, first, *refs):
    count = len(sizes)
    own_refs, other_refs, refs = refs[:count], refs[count : 2 * count], refs[2 * count :]
    weight_ref, refs = refs[0], refs[1:]
    if first:
        down_ref, refs = refs[0], refs[1:]
    send_refs, keep_refs = refs[:count], refs[count : 2 * count]
    rows_ref, hidden_ref = refs[-3:-1] if first else refs[-2:]
    if first:
        weight_ref = refs[2 * count]
    width = own_refs[0].shape[1]
    units = hidden_ref.shape[1]
    tile = weight_ref.shape[1]
    base = weight_ref.shape[0] - 2 * width // tile * units
    if first:
        copy, copies = column_copies(down_ref, weight_ref, base, refs[-1])
        for index in range(copies):
            copy(index).start()
    me = lax.axis_index("etp")
    mine = pl.ds(pl.multiple_of(me * width, width), width)
    theirs = pl.ds(pl.multiple_of((1 - me) * width, width), width)
    row = 0
    for own_ref, other_ref, size in zip(own_refs, other_refs, sizes):
        rows_ref[row : row + size, mine] = own_ref[...]
        rows_ref[row : row + size, theirs] = other_ref[...]
        row += size

    def up_step(index, carry):
        cols = pl.ds(pl.multiple_of(index * tile, tile), tile)
        source = pl.ds(pl.multiple_of(index * 2 * width, 2 * width), 2 * width)
        up_proj = jnp.dot(rows_ref[...], weight_ref[source], preferred_element_type=jnp.float32)
        hidden_ref[:, cols] = (up_proj / (1.0 + jnp.exp(-up_proj))).astype(hidden_ref.dtype)
        return carry

    lax.fori_loop(0, units // tile, up_step, 0)

    def down_piece(index, half, out_refs):
        cols = pl.ds(pl.multiple_of(index * tile, tile), tile)
        position = half * (width // tile) + index
        if first:
            copy(position).wait()
        start = base + position * units
        source = pl.ds(pl.multiple_of(start, math.gcd(base, units)), units)
        sums = jnp.dot(hidden_ref[...], weight_ref[source], preferred_element_type=jnp.float32)
        row = 0
        for out_ref, size in zip(out_refs, sizes):
            out_ref[:, cols] = sums[row : row + size].astype(out_ref.dtype)
            row += size

    def send_step(index, carry):
        down_piece(index, 1 - me, send_refs)
        return carry

    def keep_step(index, carry):
        down_piece(index, me, keep_refs)
        return carry

    lax.fori_loop(0, width // tile, send_step, 0)
    lax.fori_loop(0, width // tile, keep_step, 0)


def expert(own, other, weight, units, down_weight=None):
    sizes = [piece.shape[0] for piece in own]
    rows, width = sum(sizes), own[0].shape[1]
    count = len(sizes)
    first = down_weight is not None
    outs = [jax.ShapeDtypeStruct((size, width), own[0].dtype) for size in sizes * 2]
    scratch = [pltpu.VMEM((rows, 2 * width), own[0].dtype), pltpu.VMEM((rows, units), own[0].dtype)]
    operands = [*own, *other, *hold([weight])]
    specs = {}
    if first:
        outs.append(pltpu.VMEM(weight.shape, weight.dtype))
        scratch.append(pltpu.SemaphoreType.DMA((2 * width // weight.shape[1],)))
        operands.append(pltpu.with_memory_space_constraint(down_weight, pltpu.HBM))
        specs["in_specs"] = [VMEM] * (2 * count + 1) + [HBM]
        specs["input_output_aliases"] = {2 * count: 2 * count}
    results = call(
        functools.partial(expert_kernel, sizes, first),
        outs,
        scratch,
        flops=8 * rows * width * units,
        moved=8 * width * units,
        **specs,
    )(*operands)
    return results[:count], results[count : 2 * count], results[2 * count :]


def add_kernel(keep_ref, other_ref, *refs):
    sum_ref = refs[-1]
    total = keep_ref[...].astype(jnp.float32) + other_ref[...].astype(jnp.float32)
    sum_ref[...] = total.astype(sum_ref.dtype)


def add(keep, other, held):
    size = keep.size
    return call(
        add_kernel, [jax.ShapeDtypeStruct(other.shape, other.dtype)], flops=size, moved=8 * size
    )(keep, other, *hold(held))[0]


def mix_kernel(starts, first, table_ref, *refs):
    out_ref = refs[-1]
    row_refs = refs[: len(starts)]
    rows = table_ref.shape[0]
    total = None if first else refs[len(starts)][...]
    for start, row_ref in zip(starts, row_refs):
        places = lax.broadcasted_iota(jnp.int32, (rows, row_ref.shape[0]), 1) + start
        for k in range(2):
            taking = (table_ref[:, k : k + 1].astype(jnp.int32) == places).astype(jnp.float32).astype(jnp.bfloat16)
            taken = jnp.dot(taking, row_ref[...], preferred_element_type=jnp.float32)
            term = table_ref[:, k + 2 : k + 3] * taken
            total = term if total is None else total + term
    out_ref[...] = total.astype(out_ref.dtype)


def mix(table, parts, starts, total, dtype):
    rows, width = table.shape[0], parts[0].shape[1]
    count = sum(part.shape[0] for part in parts)
    return call(
        functools.partial(mix_kernel, starts, total is None),
        [jax.ShapeDtypeStruct((rows, width), dtype)],
        flops=4 * rows * width * count,
        moved=4 * rows * width,
    )(table, *parts, *([] if total is None else [total]))[0]


def cut(capacity, parts):
    if parts == 1 or capacity < 32:
        return [capacity]
    half = (capacity + 31) // 32 * 16
    return [half, capacity - half]


def local(tokens, experts, mixing, up_weight, down_weight):
    tok_rows = experts.shape[0]
    groups = lax.axis_size("expert")
    halves = lax.axis_size("etp")
    capacity = 2 * tok_rows // groups * 11 // 8
    up_slab = up_weight[0]
    down_slab = down_weight[0]
    paired = halves == 2

    def across(rows, offset):
        pairs = [(i, i ^ offset) for i in range(groups)]
        return rows if offset == 0 else lax.ppermute(rows, "expert", pairs)

    def swap(rows):
        return lax.ppermute(rows, "etp", [(0, 1), (1, 0)])

    def exchange(rows):
        gathered = lax.all_gather(rows, "etp", axis=1, tiled=True)
        up_proj = jnp.dot(gathered, up_slab, preferred_element_type=jnp.float32)
        hidden = jax.nn.silu(up_proj).astype(jnp.bfloat16)
        sums = jnp.dot(hidden, down_slab, preferred_element_type=jnp.float32)
        own = lax.psum_scatter(sums, "etp", scatter_dimension=1, tiled=True)
        return own.astype(jnp.bfloat16)

    tuned = paired and groups == len(MIX)
    batches = BATCHES if tuned else [[(k, 0)] for k in range(groups)]
    split = SPLIT if tuned else {}
    spans = {}
    for offset in range(groups):
        start = offset * capacity
        for index, size in enumerate(cut(capacity, split.get(offset, 1))):
            spans[offset, index] = (start, size)
            start += size
    table, *outgoing = send_rows(experts, mixing, tokens, capacity, list(spans.values()))
    outgoing = dict(zip(spans, outgoing))
    if paired:
        held = load(up_slab, down_slab, [outgoing[0, 0]])
    arrived = {(k, i): across(rows, k) for (k, i), rows in outgoing.items()}
    returned = {}
    for number, batch in enumerate(batches):
        own = [arrived[key] for key in batch]
        if paired:
            others = [swap(arrived[k, i]) for k, i in batch]
            more = [] if number else [down_slab]
            send, keep, filled = expert(own, others, held, up_slab.shape[1], *more)
            held = filled[0] if filled else held
            last = number == len(batches) - 1
            own = []
            for (k, i), mine, rows in zip(batch, keep, send):
                other = swap(rows)
                kept = [held] if (k, i) in HOLD and not last else []
                own.append(add(mine, other, kept))
        else:
            own = [exchange(rows) for rows in own]
        for (k, i), rows in zip(batch, own):
            returned[k, i] = across(rows, k)
    total = None
    order = MIX if tuned else range(groups)
    for offset in order:
        keys = [key for key in spans if key[0] == offset]
        total = mix(
            table,
            [returned[key] for key in keys],
            [spans[key][0] for key in keys],
            total,
            tokens.dtype if offset == order[-1] else jnp.float32,
        )
    return total


def solution(mesh):
    placed = (
        P(("dp", "expert"), "etp"),
        P(("dp", "expert"), None),
        P(("dp", "expert"), None),
        P("expert", None, "etp"),
        P("expert", "etp", None),
    )

    return jax.shard_map(
        local, mesh=mesh, in_specs=placed, out_specs=P(("dp", "expert"), "etp"), check_vma=False
    )
```

```python
import functools
import math

import jax
import jax.numpy as jnp
from jax import lax
from jax.experimental import pallas as pl
from jax.experimental.pallas import tpu as pltpu
from jax.sharding import PartitionSpec as P


VMEM = pl.BlockSpec(memory_space=pltpu.VMEM)
ANY = pl.BlockSpec(memory_space=pl.ANY)
HBM = pl.BlockSpec(memory_space=pltpu.HBM)
GRANT = 12 * 1024 * 1024
BATCHES = (((0, 0), (2, 0)), ((2, 1), (1, 0)), ((3, 0), (3, 1)))
MIX = (2, 1, 0, 3)
SPLIT = {2: 2, 3: 2}
HOLD = ((2, 0), (2, 1))


def hold(arrays):
    return [pltpu.with_memory_space_constraint(array, pltpu.VMEM) for array in arrays]


def call(body, outs, scratch=(), flops=0, moved=0, grant=GRANT, **specs):
    return pl.pallas_call(
        body,
        out_specs=[VMEM] * len(outs),
        out_shape=outs,
        scratch_shapes=scratch,
        compiler_params=pltpu.CompilerParams(vmem_limit_bytes=grant),
        cost_estimate=pl.CostEstimate(flops=flops, bytes_accessed=moved, transcendentals=0),
        **specs,
    )


def tile_of(size):
    for tile in (512, 384, 256, 128):
        if size % tile == 0:
            return tile
    return size


def send_kernel(layout, *refs):
    capacity, pieces = layout
    sources, table_ref, out_refs = refs[:3], refs[3], refs[4:-4]
    copies = [
        pltpu.make_async_copy(source, target, refs[-1].at[index])
        for index, (source, target) in enumerate(zip(sources, refs[-4:-1]))
    ]
    for copy in copies:
        copy.start()
    for copy in copies:
        copy.wait()
    experts_ref, mixing_ref, tokens_ref = refs[-4:-1]
    rows = tokens_ref.shape[0]
    me = lax.axis_index("expert")
    first = experts_ref[0:1, :]
    second = experts_ref[1:2, :]
    earlier = lax.broadcasted_iota(jnp.int32, (rows, rows), 0) < lax.broadcasted_iota(
        jnp.int32, (rows, rows), 1
    )
    earlier = earlier.astype(jnp.float32).astype(jnp.bfloat16)
    offsets = sorted({start // capacity for start, _ in pieces})
    first_slot = jnp.zeros((1, rows), jnp.int32)
    second_slot = jnp.zeros((1, rows), jnp.int32)
    for offset in offsets:
        expert = me ^ offset
        named = (first == expert) | (second == expert)
        marks = jnp.broadcast_to(named.astype(jnp.float32), (16, rows)).astype(jnp.bfloat16)
        rank = jnp.dot(marks, earlier, preferred_element_type=jnp.float32)[0:1, :]
        slot = rank.astype(jnp.int32) + offset * capacity
        first_slot = jnp.where(first == expert, slot, first_slot)
        second_slot = jnp.where(second == expert, slot, second_slot)
        slot = jnp.where(named, slot, -1)
        for (start, size), out_ref in zip(pieces, out_refs):
            if start // capacity == offset:
                places = lax.broadcasted_iota(jnp.int32, (size, rows), 0) + start
                placing = (slot == places).astype(jnp.float32).astype(jnp.bfloat16)
                out_ref[...] = jnp.dot(
                    placing, tokens_ref[...], preferred_element_type=jnp.float32
                ).astype(out_ref.dtype)
    lines = [
        first_slot.astype(jnp.float32),
        second_slot.astype(jnp.float32),
        mixing_ref[0:1, :],
        mixing_ref[1:2, :],
        jnp.zeros((124, rows), jnp.float32),
    ]
    table_ref[...] = jnp.concatenate(lines, axis=0).T


def send_rows(experts, mixing, tokens, capacity, pieces):
    rows, width = tokens.shape
    outs = [jax.ShapeDtypeStruct((rows, 128), jnp.float32)]
    outs += [jax.ShapeDtypeStruct((size, width), tokens.dtype) for _, size in pieces]
    sources = (experts.T, mixing.T, tokens)
    scratch = [pltpu.VMEM(x.shape, x.dtype) for x in sources]
    return call(
        functools.partial(send_kernel, (capacity, pieces)),
        outs,
        [*scratch, pltpu.SemaphoreType.DMA((3,))],
        flops=2 * rows * width * sum(size for _, size in pieces),
        moved=4 * rows * width,
        grant=12 * 1024 * 1024,
        in_specs=[HBM] * 3,
    )(*[pltpu.with_memory_space_constraint(x, pltpu.HBM) for x in sources])


def column_copies(source_ref, held_ref, base, sems):
    size, tile = source_ref.shape[0], held_ref.shape[1]

    def copy(index):
        cols = pl.ds(pl.multiple_of(index * tile, tile), tile)
        rows = pl.ds(pl.multiple_of(base + index * size, math.gcd(base, size)), size)
        return pltpu.make_async_copy(source_ref.at[:, cols], held_ref.at[rows], sems.at[index])

    return copy, source_ref.shape[1] // tile


def load_kernel(up_ref, *refs):
    held_ref, sems = refs[-2:]
    copy, count = column_copies(up_ref, held_ref, 0, sems)
    for index in range(count):
        copy(index).start()
    for index in range(count):
        copy(index).wait()


def load(up_weight, down_weight, after):
    tile = tile_of(math.gcd(up_weight.shape[1], down_weight.shape[1] // 2))
    size = up_weight.size + down_weight.size
    source = pltpu.with_memory_space_constraint(up_weight, pltpu.HBM)
    return call(
        load_kernel,
        [pltpu.VMEM((size // tile, tile), up_weight.dtype)],
        [pltpu.SemaphoreType.DMA((up_weight.shape[1] // tile,))],
        moved=2 * up_weight.size,
        flops=8 * 10**9,
        in_specs=[HBM] + [ANY] * len(after),
    )(source, *after)[0]


def expert_kernel(sizes, first, *refs):
    count = len(sizes)
    own_refs, other_refs, refs = refs[:count], refs[count : 2 * count], refs[2 * count :]
    weight_ref, refs = refs[0], refs[1:]
    if first:
        down_ref, refs = refs[0], refs[1:]
    send_refs, keep_refs = refs[:count], refs[count : 2 * count]
    rows_ref, hidden_ref = refs[-3:-1] if first else refs[-2:]
    if first:
        weight_ref = refs[2 * count]
    width = own_refs[0].shape[1]
    units = hidden_ref.shape[1]
    tile = weight_ref.shape[1]
    base = weight_ref.shape[0] - 2 * width // tile * units
    if first:
        copy, copies = column_copies(down_ref, weight_ref, base, refs[-1])
        for index in range(copies):
            copy(index).start()
    me = lax.axis_index("etp")
    mine = pl.ds(pl.multiple_of(me * width, width), width)
    theirs = pl.ds(pl.multiple_of((1 - me) * width, width), width)
    row = 0
    for own_ref, other_ref, size in zip(own_refs, other_refs, sizes):
        rows_ref[row : row + size, mine] = own_ref[...]
        rows_ref[row : row + size, theirs] = other_ref[...]
        row += size

    def up_step(index, carry):
        cols = pl.ds(pl.multiple_of(index * tile, tile), tile)
        source = pl.ds(pl.multiple_of(index * 2 * width, 2 * width), 2 * width)
        up_proj = jnp.dot(rows_ref[...], weight_ref[source], preferred_element_type=jnp.float32)
        hidden_ref[:, cols] = (up_proj / (1.0 + jnp.exp(-up_proj))).astype(hidden_ref.dtype)
        return carry

    lax.fori_loop(0, units // tile, up_step, 0)

    def down_piece(index, half, out_refs):
        cols = pl.ds(pl.multiple_of(index * tile, tile), tile)
        position = half * (width // tile) + index
        if first:
            copy(position).wait()
        start = base + position * units
        source = pl.ds(pl.multiple_of(start, math.gcd(base, units)), units)
        sums = jnp.dot(hidden_ref[...], weight_ref[source], preferred_element_type=jnp.float32)
        row = 0
        for out_ref, size in zip(out_refs, sizes):
            out_ref[:, cols] = sums[row : row + size].astype(out_ref.dtype)
            row += size

    def send_step(index, carry):
        down_piece(index, 1 - me, send_refs)
        return carry

    def keep_step(index, carry):
        down_piece(index, me, keep_refs)
        return carry

    lax.fori_loop(0, width // tile, send_step, 0)
    lax.fori_loop(0, width // tile, keep_step, 0)


def expert(own, other, weight, units, down_weight=None):
    sizes = [piece.shape[0] for piece in own]
    rows, width = sum(sizes), own[0].shape[1]
    count = len(sizes)
    first = down_weight is not None
    outs = [jax.ShapeDtypeStruct((size, width), own[0].dtype) for size in sizes * 2]
    scratch = [pltpu.VMEM((rows, 2 * width), own[0].dtype), pltpu.VMEM((rows, units), own[0].dtype)]
    operands = [*own, *other, *hold([weight])]
    specs = {}
    if first:
        outs.append(pltpu.VMEM(weight.shape, weight.dtype))
        scratch.append(pltpu.SemaphoreType.DMA((2 * width // weight.shape[1],)))
        operands.append(pltpu.with_memory_space_constraint(down_weight, pltpu.HBM))
        specs["in_specs"] = [VMEM] * (2 * count + 1) + [HBM]
        specs["input_output_aliases"] = {2 * count: 2 * count}
    results = call(
        functools.partial(expert_kernel, sizes, first),
        outs,
        scratch,
        flops=8 * rows * width * units,
        moved=8 * width * units,
        **specs,
    )(*operands)
    return results[:count], results[count : 2 * count], results[2 * count :]


def add_kernel(keep_ref, other_ref, *refs):
    sum_ref = refs[-1]
    total = keep_ref[...].astype(jnp.float32) + other_ref[...].astype(jnp.float32)
    sum_ref[...] = total.astype(sum_ref.dtype)


def add(keep, other, held):
    size = keep.size
    return call(
        add_kernel, [jax.ShapeDtypeStruct(other.shape, other.dtype)], flops=size, moved=8 * size
    )(keep, other, *hold(held))[0]


def mix_kernel(starts, first, table_ref, *refs):
    out_ref = refs[-1]
    row_refs = refs[: len(starts)]
    rows = table_ref.shape[0]
    total = None if first else refs[len(starts)][...]
    for start, row_ref in zip(starts, row_refs):
        places = lax.broadcasted_iota(jnp.int32, (rows, row_ref.shape[0]), 1) + start
        for k in range(2):
            taking = (table_ref[:, k : k + 1].astype(jnp.int32) == places).astype(jnp.float32).astype(jnp.bfloat16)
            taken = jnp.dot(taking, row_ref[...], preferred_element_type=jnp.float32)
            term = table_ref[:, k + 2 : k + 3] * taken
            total = term if total is None else total + term
    out_ref[...] = total.astype(out_ref.dtype)


def mix(table, parts, starts, total, dtype):
    rows, width = table.shape[0], parts[0].shape[1]
    count = sum(part.shape[0] for part in parts)
    return call(
        functools.partial(mix_kernel, starts, total is None),
        [jax.ShapeDtypeStruct((rows, width), dtype)],
        flops=4 * rows * width * count,
        moved=4 * rows * width,
    )(table, *parts, *([] if total is None else [total]))[0]


def cut(capacity, parts):
    if parts == 1 or capacity < 32:
        return [capacity]
    half = (capacity + 31) // 32 * 16
    return [half, capacity - half]


def local(tokens, experts, mixing, up_weight, down_weight):
    tok_rows = experts.shape[0]
    groups = lax.axis_size("expert")
    halves = lax.axis_size("etp")
    capacity = 2 * tok_rows // groups * 11 // 8
    up_slab = up_weight[0]
    down_slab = down_weight[0]
    paired = halves == 2

    def across(rows, offset):
        pairs = [(i, i ^ offset) for i in range(groups)]
        return rows if offset == 0 else lax.ppermute(rows, "expert", pairs)

    def swap(rows):
        return lax.ppermute(rows, "etp", [(0, 1), (1, 0)])

    def exchange(rows):
        gathered = lax.all_gather(rows, "etp", axis=1, tiled=True)
        up_proj = jnp.dot(gathered, up_slab, preferred_element_type=jnp.float32)
        hidden = jax.nn.silu(up_proj).astype(jnp.bfloat16)
        sums = jnp.dot(hidden, down_slab, preferred_element_type=jnp.float32)
        own = lax.psum_scatter(sums, "etp", scatter_dimension=1, tiled=True)
        return own.astype(jnp.bfloat16)

    tuned = paired and groups == len(MIX)
    batches = BATCHES if tuned else [[(k, 0)] for k in range(groups)]
    split = SPLIT if tuned else {}
    spans = {}
    for offset in range(groups):
        start = offset * capacity
        for index, size in enumerate(cut(capacity, split.get(offset, 1))):
            spans[offset, index] = (start, size)
            start += size
    table, *outgoing = send_rows(experts, mixing, tokens, capacity, list(spans.values()))
    outgoing = dict(zip(spans, outgoing))
    if paired:
        held = load(up_slab, down_slab, [outgoing[0, 0]])
    arrived = {(k, i): across(rows, k) for (k, i), rows in outgoing.items()}
    returned = {}
    for number, batch in enumerate(batches):
        own = [arrived[key] for key in batch]
        if paired:
            others = [swap(arrived[k, i]) for k, i in batch]
            more = [] if number else [down_slab]
            send, keep, filled = expert(own, others, held, up_slab.shape[1], *more)
            held = filled[0] if filled else held
            last = number == len(batches) - 1
            own = []
            for (k, i), mine, rows in zip(batch, keep, send):
                other = swap(rows)
                kept = [held] if (k, i) in HOLD and not last else []
                own.append(add(mine, other, kept))
        else:
            own = [exchange(rows) for rows in own]
        for (k, i), rows in zip(batch, own):
            returned[k, i] = across(rows, k)
    total = None
    order = MIX if tuned else range(groups)
    for offset in order:
        keys = [key for key in spans if key[0] == offset]
        total = mix(
            table,
            [returned[key] for key in keys],
            [spans[key][0] for key in keys],
            total,
            tokens.dtype if offset == order[-1] else jnp.float32,
        )
    return total


def solution(mesh):
    placed = (
        P(("dp", "expert"), "etp"),
        P(("dp", "expert"), None),
        P(("dp", "expert"), None),
        P("expert", None, "etp"),
        P("expert", "etp", None),
    )

    return jax.shard_map(
        local, mesh=mesh, in_specs=placed, out_specs=P(("dp", "expert"), "etp"), check_vma=False
    )
```
